256 devices in a mesh: bank: 32 (over z_hi, y, x), lane: 8 (over z_lo, core).
Axes of the slice: x: 4, y: 4, z: 8 (z_hi: 2, z_lo: 4; z = z_hi * 4 + z_lo), core: 2. Of those that a mesh axis runs over, the one named last changes fastest.
Arguments:
- amplitudes: float32 [2, 1024, 128, 128], P(None, ('bank', 'lane')), may hold values from -6 to 6
- energies: float32 [1024, 128, 128], P(('bank', 'lane')), may hold values from -2 to 2
- phase_angles: float32 [2, 128], replicated, may hold values from 0.3 to 1.2
- mix_angles: float32 [2, 4], replicated, may hold values from 0.3 to 1.2
Outputs:
- final_parts: float32 [2, 1024, 128, 128], P(None, ('bank', 'lane'))
- marginal: float32 [32, 128, 128], P('lane', 'bank')
The draws below stay inside these ranges and needn't reach their ends.
All inputs are finite; a program needn't handle non-finite values.
Results may differ from the reference program's by a relative error of at most 0.0003.
Values sent between devices are 32-bit elements; how exact they have to be, the bound alone decides.
A program may use at most 64 MiB of HBM per device.

```python
import jax
import jax.numpy as jnp
from jax import lax

BLOCKS_DEV = 4
ROWS = 128
LANES = 128
BLOCKS = 1024
LAYERS = 2
N_BANK = 32
N_LANE = 8


def steps_of(stream_key, dims, pieces, low, top_value):
    def one(axis_at, shards_of):
        heights = jax.random.uniform(jax.random.fold_in(jax.random.fold_in(stream_key, 6), axis_at), (shards_of,), jnp.float32, low / len(pieces), top_value / len(pieces))
        return jnp.repeat(jnp.exp(heights), dims[axis_at] // shards_of).reshape((-1,) + (1,) * (len(dims) - axis_at - 1))

    loudness = one(*pieces[0])
    for cut in pieces[1:]:
        loudness = loudness * one(*cut)
    return loudness


def noise(key, dims, spread, bound, shards=(), kind=jnp.bfloat16):
    entries = jax.random.normal(key, dims, jnp.float32) * spread
    if len(shards) > 0:
        entries = steps_of(key, dims, shards, -0.22, 0.18) * entries
    return jnp.clip(entries, min=-bound, max=bound).astype(kind)


def setup_inputs(seed: int = 0) -> dict:
    key_list = jax.random.split(jax.random.key(seed), 5)
    return {
        "amplitudes": noise(key_list[0], (2, BLOCKS, ROWS, LANES), 1.0, 6.0, ((1, 256),), jnp.float32),
        "energies": jnp.clip(jax.random.uniform(key_list[1], (BLOCKS, ROWS, LANES), jnp.float32, -2.0, 2.0) * steps_of(key_list[1], (BLOCKS, ROWS, LANES), ((0, 256),), -0.4, 0.0), -2.0, 2.0),
        "phase_angles": jnp.clip(jax.random.uniform(key_list[2], (LAYERS, LANES), jnp.float32, 0.3, 1.2), 0.3, 1.2),
        "mix_angles": jnp.clip(jax.random.uniform(key_list[3], (LAYERS, 4), jnp.float32, 0.3, 1.2), 0.3, 1.2),
    }


def count_bits(values, count):
    places = jnp.arange(count.bit_length() - 1, dtype=jnp.int32)
    return jnp.sum((values[..., None] >> places) & 1, axis=-1)


def turn_table(count, angle):
    rank = jnp.arange(count, dtype=jnp.int32)
    apart = count_bits(rank[:, None] ^ rank[None, :], count)
    bits = count.bit_length() - 1
    size = jnp.cos(angle) ** (bits - apart).astype(jnp.float32) * jnp.sin(angle) ** apart.astype(jnp.float32)
    real_sign = jnp.where(apart % 4 == 0, 1.0, jnp.where(apart % 4 == 2, -1.0, 0.0)).astype(jnp.float32)
    imag_sign = jnp.where(apart % 4 == 1, -1.0, jnp.where(apart % 4 == 3, 1.0, 0.0)).astype(jnp.float32)
    return size * real_sign, size * imag_sign


def apply_along(values, dim, angle):
    real_part, imag_part = turn_table(values.shape[dim], angle)
    def times(table):
        moved = jnp.tensordot(values, table, axes=([dim], [0]), precision=lax.Precision.HIGHEST)
        return jnp.moveaxis(moved, -1, dim)
    by_real = times(real_part)
    by_imag = times(imag_part)
    return jnp.stack([by_real[0] - by_imag[1], by_real[1] + by_imag[0]])


def diagonal_step(values, levels, angle):
    turn = angle * levels
    return jnp.stack([values[0] * jnp.cos(turn) + values[1] * jnp.sin(turn), values[1] * jnp.cos(turn) - values[0] * jnp.sin(turn)])


def reference(amplitudes, energies, phase_angles, mix_angles):
    values = amplitudes
    for layer in range(LAYERS):
        values = diagonal_step(values, energies, phase_angles[layer])
        values = apply_along(values, 3, mix_angles[layer, 0])
        values = apply_along(values, 2, mix_angles[layer, 1])
        parts = values.reshape(2, N_BANK, N_LANE, BLOCKS_DEV, ROWS, LANES)
        parts = apply_along(parts, 1, mix_angles[layer, 2])
        parts = apply_along(parts, 2, mix_angles[layer, 3])
        parts = apply_along(parts, 3, mix_angles[layer, 2])
        values = parts.reshape(values.shape)
    chance = values[0] * values[0] + values[1] * values[1]
    marginal = jnp.mean(chance.reshape(N_BANK, -1, ROWS, LANES), axis=0)
    return values, marginal
```

```python
import functools

import jax
import jax.numpy as jnp
from jax import lax
from jax.experimental import pallas as pl
from jax.experimental.pallas import tpu as pltpu
from jax.sharding import PartitionSpec as P

MESH = pl.DeviceIdType.MESH
F32 = jnp.float32
BF16 = jnp.bfloat16

Z_STEPS = (4, 3, 5, 2, 6, 1, 7)
XY_STEPS = tuple((dx, dy) for dx in (2, 1, 3, 0) for dy in (2, 1, 3, 0) if dx or dy)
STAGES = 20


def sine_cosine(angle):
    half = 0.5 * angle
    w = half * half
    s = jnp.full_like(w, -1.0 / 39916800.0)
    for term in (1.0 / 362880.0, -1.0 / 5040.0, 1.0 / 120.0, -1.0 / 6.0, 1.0):
        s = s * w + term
    s = s * half
    c = jnp.full_like(w, 1.0 / 479001600.0)
    for term in (-1.0 / 3628800.0, 1.0 / 40320.0, -1.0 / 720.0, 1.0 / 24.0, -0.5, 1.0):
        c = c * w + term
    return 2.0 * s * c, 1.0 - 2.0 * s * s


def split(value):
    high = value.astype(BF16)
    return high, (value - high.astype(F32)).astype(BF16)


def times(left, right):
    (lh, ll), (rh, rl) = left, right
    dot = functools.partial(jnp.dot, preferred_element_type=F32)
    return dot(lh, rh) + dot(lh, rl) + dot(ll, rh)


def kernel(amps, energies, phases, mixes, out, marg, *scratch):
    (tables, canon, moved, other, e_send, e_mid, e_got, s_buf, s_mid, s_got, t_buf, t_mid, t_oth, t_mix, t_got,
     held, p_send, p_got, p_sum, p_far, send_sem, recv_sem) = scratch
    bank, lane = lax.axis_index("bank"), lax.axis_index("lane")
    x, y, z_hi = bank % 4, (bank // 4) % 4, bank // 16
    z, core = z_hi * 4 + lane // 2, lane % 2
    xy = y * 4 + x

    def z_peer(step):
        there = (z + step) % 8
        return there, ((there // 4) * 16 + xy, (there % 4) * 2 + core)

    def xy_peer(step):
        there = ((y + step[1]) % 4) * 4 + (x + step[0]) % 4
        return there, (z_hi * 16 + there, lane)

    partner = (bank, (lane // 2) * 2 + 1 - core)
    z_peers = [z_peer(step) for step in Z_STEPS]
    xy_peers = [xy_peer(step) for step in XY_STEPS]

    def remote(src, dst, stage, device):
        return pltpu.make_async_remote_copy(
            src_ref=src, dst_ref=dst, send_sem=send_sem.at[stage], recv_sem=recv_sem.at[stage],
            device_id=device, device_id_type=MESH,
        )

    def send_z(src, dst, stage):
        for there, device in z_peers:
            remote(src.at[there], dst.at[z], stage, device).start()
        dst[z] = src[z]

    def send_xy(src, dst, stage, unit):
        for there, device in xy_peers:
            remote(
                src.at[:, pl.ds(pl.multiple_of(there * unit, unit), unit), :],
                dst.at[:, pl.ds(pl.multiple_of(xy * unit, unit), unit), :],
                stage, device,
            ).start()
        own = pl.ds(pl.multiple_of(xy * unit, unit), unit)
        dst[:, own, :] = src[:, own, :]

    def all_of(ref, sem):
        return pltpu.make_async_copy(ref, ref, sem)

    def z_bytes(buf):
        return buf.at[pl.ds(0, 7)]

    def xy_bytes(buf, unit):
        return buf.at[:, pl.ds(0, 15 * unit), :]

    barrier = pltpu.get_barrier_semaphore()
    for _, device in z_peers + xy_peers:
        pl.semaphore_signal(barrier, inc=1, device_id=device, device_id_type=MESH)
    pl.semaphore_signal(barrier, inc=1, device_id=partner, device_id_type=MESH)

    for r0 in range(2):
        for sz in range(8):
            for r1 in range(2):
                e_send[r0, sz, pl.ds(r1, 16, stride=2), :] = energies[
                    sz // 2, pl.ds((sz % 2) * 64 + 2 * r1 + r0, 16, stride=4), :
                ]
    pl.semaphore_wait(barrier, 23)
    send_z(e_send.at[0], e_mid.at[0], 0)
    send_xy(e_send.at[1], e_mid.at[1], 1, 2)

    mix_sin, mix_cos = sine_cosine(mixes[...])

    def cs(layer, group, shape):
        at = (slice(layer, layer + 1), slice(group, group + 1))
        return jnp.broadcast_to(mix_cos[at], shape), jnp.broadcast_to(mix_sin[at], shape)

    row = lax.broadcasted_iota(jnp.int32, (128, 128), 0)
    column = lax.broadcasted_iota(jnp.int32, (128, 128), 1)
    apart = row ^ column

    def build(slot, layer, groups, on_left):
        size, count = None, None
        for k, group in enumerate(groups):
            c, s = cs(layer, group, (128, 128))
            bit = (apart >> k) & 1
            factor = jnp.where(bit == 1, s, c)
            size = factor if size is None else size * factor
            count = bit if count is None else count + bit
        odd = (count & 1) == 1
        sign = 1.0 - (count & 2).astype(F32)
        re = jnp.where(odd, 0.0, size * sign)
        im = jnp.where(odd, -size * sign, 0.0)
        for half, (real, imag) in enumerate(zip(split(re), split(im))):
            tables[slot, half, 0:128, 0:128] = real
            tables[slot, half, 128:256, 128:256] = real
            tables[slot, half, 0:128, 128:256] = -imag if on_left else imag
            tables[slot, half, 128:256, 0:128] = imag if on_left else -imag

    def table(slot):
        return tables[slot, 0], tables[slot, 1]

    lanes = (0,) * 7
    rows = (1,) * 5 + (2, 2)
    chips = (2,) * 4 + (3, 3) + (2,)
    build(0, 0, lanes, False)
    build(1, 0, rows, True)

    def turned(re, im, levels, layer):
        angle = jnp.broadcast_to(phases[layer:layer + 1, :], levels.shape) * levels
        s, c = sine_cosine(angle)
        return re * c + im * s, im * c - re * s

    def mixed(u, v, c, s):
        (ur, ui), (vr, vi) = u, v
        return (c * ur + s * vi, c * ui - s * vr), (c * vr + s * ui, c * vi - s * ur)

    shape = (32, 128)
    c1, s1 = cs(0, 1, shape)
    for t in range(4):
        parts = {}
        for q in range(4):
            at = pl.ds(q, 32, stride=4)
            parts[q] = turned(amps[0, t, at, :], amps[1, t, at, :], energies[t, at, :], 0)
        for low, high in ((0, 1), (2, 3), (0, 2), (1, 3)):
            parts[low], parts[high] = mixed(parts[low], parts[high], c1, s1)
        for q in range(4):
            place = ((q % 2) * 2 + q // 2) * 128 + t * 32
            canon[place:place + 32, 0:128] = parts[q][0]
            canon[place:place + 32, 128:256] = parts[q][1]
    for r0 in range(2):
        done = times(split(canon[r0 * 256:r0 * 256 + 256, :]), table(0))
        for r1 in range(2):
            for part in range(2):
                moved[r0, part * 128:part * 128 + 128, r1 * 128:r1 * 128 + 128] = done[
                    r1 * 128:r1 * 128 + 128, part * 128:part * 128 + 128
                ]
        remote(moved.at[r0], other.at[r0], 2 + r0, partner).start()

    def spread(buf, r0, value):
        for sz in range(8):
            for part in range(2):
                for r1 in range(2):
                    buf[r0, sz, pl.ds(2 * part + r1, 16, stride=4), :] = value[
                        part * 128 + sz * 16:part * 128 + sz * 16 + 16, r1 * 128:r1 * 128 + 128
                    ]

    def gathered(buf, r0):
        columns = []
        for r1 in range(2):
            columns.append(jnp.concatenate(
                [buf[r0, sz, pl.ds(2 * part + r1, 16, stride=4), :] for part in range(2) for sz in range(8)], axis=0
            ))
        return jnp.concatenate(columns, axis=1)

    c3, s3 = cs(0, 3, (128, 256))
    for r0 in range(2):
        all_of(other.at[r0], recv_sem.at[2 + r0]).wait()
        re = c3 * moved[r0, 0:128, :] + s3 * other[r0, 128:256, :]
        im = c3 * moved[r0, 128:256, :] - s3 * other[r0, 0:128, :]
        spread(s_buf, r0, times(table(1), split(jnp.concatenate([re, im], axis=0))))
        if r0 == 0:
            send_z(s_buf.at[0], s_mid.at[0], 4)
        else:
            send_xy(s_buf.at[1], s_mid.at[1], 5, 4)

    all_of(z_bytes(e_mid.at[0]), recv_sem.at[0]).wait()
    send_xy(e_mid.at[0], e_got.at[0], 6, 2)
    all_of(xy_bytes(e_mid.at[1], 2), recv_sem.at[1]).wait()
    send_z(e_mid.at[1], e_got.at[1], 7)

    all_of(xy_bytes(s_mid.at[1], 4), recv_sem.at[5]).wait()
    send_z(s_mid.at[1], s_got.at[1], 8)
    build(2, 0, chips, True)
    build(3, 1, chips, True)
    all_of(z_bytes(s_mid.at[0]), recv_sem.at[4]).wait()
    send_xy(s_mid.at[0], s_got.at[0], 9, 4)
    build(4, 1, lanes, False)
    build(5, 1, rows, True)

    def middle(r0):
        value = times(table(2), split(gathered(s_got, r0)))
        c, s = cs(1, 1, (128, 128))
        parts = []
        for r1 in range(2):
            levels = jnp.concatenate([e_got[r0, sz, pl.ds(r1, 16, stride=2), :] for sz in range(8)], axis=0)
            at = slice(r1 * 128, r1 * 128 + 128)
            parts.append(turned(value[0:128, at], value[128:256, at], levels, 1))
        parts = mixed(parts[0], parts[1], c, s)
        value = jnp.concatenate([jnp.concatenate(part, axis=1) for part in parts], axis=0)
        value = times(split(value), table(4))
        value = jnp.concatenate(
            [jnp.concatenate([value[0:128, at], value[128:256, at]], axis=1) for at in (slice(0, 128), slice(128, 256))],
            axis=0,
        )
        held[r0] = times(table(3), split(value))

    all_of(xy_bytes(e_got.at[0], 2), recv_sem.at[6]).wait()
    all_of(xy_bytes(s_got.at[0], 4), recv_sem.at[9]).wait()
    middle(0)
    all_of(z_bytes(e_got.at[1]), recv_sem.at[7]).wait()
    all_of(z_bytes(s_got.at[1]), recv_sem.at[8]).wait()
    middle(1)

    c0, s0 = cs(1, 1, (128, 256))
    first, second = mixed(
        (held[0, 0:128, :], held[0, 128:256, :]), (held[1, 0:128, :], held[1, 128:256, :]), c0, s0
    )
    spread(t_buf, 1, jnp.concatenate(second, axis=0))
    send_z(t_buf.at[1], t_mid.at[1], 10)
    spread(t_buf, 0, jnp.concatenate(first, axis=0))
    send_xy(t_buf.at[0], t_mid.at[0], 11, 4)

    ck, sk = cs(1, 3, (16, 128))

    def core_mixed(r0):
        for sz in range(8):
            for part in range(2):
                for r1 in range(2):
                    own = t_mid[r0, sz, pl.ds(2 * part + r1, 16, stride=4), :]
                    far = t_oth[r0, sz, pl.ds(2 * (1 - part) + r1, 16, stride=4), :]
                    t_mix[r0, sz, pl.ds(2 * part + r1, 16, stride=4), :] = (
                        ck * own + sk * far if part == 0 else ck * own - sk * far
                    )

    all_of(xy_bytes(t_mid.at[0], 4), recv_sem.at[11]).wait()
    remote(t_mid.at[0], t_oth.at[0], 12, partner).start()
    all_of(t_oth.at[0], recv_sem.at[12]).wait()
    core_mixed(0)
    send_z(t_mix.at[0], t_got.at[0], 13)
    all_of(z_bytes(t_mid.at[1]), recv_sem.at[10]).wait()
    remote(t_mid.at[1], t_oth.at[1], 14, partner).start()
    all_of(t_oth.at[1], recv_sem.at[14]).wait()
    core_mixed(1)
    send_xy(t_mix.at[1], t_got.at[1], 15, 4)

    def final(r0):
        value = times(table(5), split(gathered(t_got, r0)))
        for part in range(2):
            for t in range(4):
                for r1 in range(2):
                    out[part, t, pl.ds(2 * r1 + r0, 32, stride=4), :] = value[
                        part * 128 + t * 32:part * 128 + t * 32 + 32, r1 * 128:r1 * 128 + 128
                    ]
        chance = value[0:128, :] * value[0:128, :] + value[128:256, :] * value[128:256, :]
        for t in range(4):
            for r6 in range(2):
                for r1 in range(2):
                    at = t * 32 + r6 * 16
                    p_send[r6, pl.ds(t * 4 + r1 * 2 + r0, 16, stride=16), :] = chance[
                        at:at + 16, r1 * 128:r1 * 128 + 128
                    ]

    all_of(xy_bytes(t_got.at[1], 4), recv_sem.at[15]).wait()
    final(1)
    all_of(z_bytes(t_got.at[0]), recv_sem.at[13]).wait()
    final(0)

    for there, device in xy_peers:
        remote(
            p_send.at[:, pl.ds(pl.multiple_of(there * 16, 16), 16), :], p_got.at[xy], 16, device
        ).start()
    p_got[xy] = p_send[:, pl.ds(pl.multiple_of(xy * 16, 16), 16), :]
    all_of(p_got.at[pl.ds(0, 15)], recv_sem.at[16]).wait()
    total = p_got[0]
    for k in range(1, 16):
        total = total + p_got[k]
    p_sum[...] = total
    far = remote(p_sum.at[1 - z_hi], p_far, 17, ((1 - z_hi) * 16 + xy, lane))
    far.start()
    all_of(p_far, recv_sem.at[17]).wait()
    whole = (p_sum[z_hi] + p_far[...]) * (1.0 / 32.0)
    for t in range(4):
        marg[t] = whole[t * 4:t * 4 + 4, :]

    for stage, buf in (
        (0, z_bytes(e_send.at[0])), (7, z_bytes(e_mid.at[1])), (4, z_bytes(s_buf.at[0])), (8, z_bytes(s_mid.at[1])),
        (10, z_bytes(t_buf.at[1])), (13, z_bytes(t_mix.at[0])),
        (1, xy_bytes(e_send.at[1], 2)), (6, xy_bytes(e_mid.at[0], 2)),
        (5, xy_bytes(s_buf.at[1], 4)), (9, xy_bytes(s_mid.at[0], 4)), (11, xy_bytes(t_buf.at[0], 4)),
        (15, xy_bytes(t_mix.at[1], 4)),
        (2, moved.at[0]), (3, moved.at[1]), (12, t_mid.at[0]), (14, t_mid.at[1]),
        (16, p_got.at[pl.ds(0, 15)]), (17, p_far),
    ):
        all_of(buf, send_sem.at[stage]).wait()


def on_device(amplitudes, energies, phase_angles, mix_angles):
    vmem = pl.BlockSpec(memory_space=pltpu.VMEM)
    half = pltpu.VMEM((2, 8, 64, 128), F32)
    levels = pltpu.VMEM((2, 8, 32, 128), F32)
    wide = pltpu.VMEM((2, 256, 256), F32)
    return pl.pallas_call(
        kernel,
        out_shape=(
            jax.ShapeDtypeStruct((2, 4, 128, 128), F32),
            jax.ShapeDtypeStruct((4, 4, 128), F32),
        ),
        in_specs=[vmem] * 4,
        out_specs=(vmem, vmem),
        scratch_shapes=[
            pltpu.VMEM((6, 2, 256, 256), BF16),
            pltpu.VMEM((512, 256), F32),
            wide, wide,
            levels, levels, levels,
            half, half, half,
            half, half, half, half, half,
            wide,
            pltpu.VMEM((2, 256, 128), F32),
            pltpu.VMEM((16, 2, 16, 128), F32),
            pltpu.VMEM((2, 16, 128), F32),
            pltpu.VMEM((16, 128), F32),
            pltpu.SemaphoreType.DMA((STAGES,)),
            pltpu.SemaphoreType.DMA((STAGES,)),
        ],
        compiler_params=pltpu.CompilerParams(
            collective_id=0, has_side_effects=True, vmem_limit_bytes=48 * 1024 * 1024
        ),
    )(amplitudes, energies, phase_angles, mix_angles)


def solution(mesh):
    placed = (P(None, ("bank", "lane"), None, None), P(("bank", "lane"), None, None), P(), P())
    return jax.shard_map(
        on_device,
        mesh=mesh,
        in_specs=placed,
        out_specs=(P(None, ("bank", "lane"), None, None), P("lane", "bank", None)),
        check_vma=False,
    )
```

```python
import functools

import jax
import jax.numpy as jnp
from jax import lax
from jax.experimental import pallas as pl
from jax.experimental.pallas import tpu as pltpu
from jax.sharding import PartitionSpec as P

MESH = pl.DeviceIdType.MESH
F32 = jnp.float32
BF16 = jnp.bfloat16

Z_STEPS = (4, 3, 5, 2, 6, 1, 7)
XY_STEPS = tuple((dx, dy) for dx in (2, 1, 3, 0) for dy in (2, 1, 3, 0) if dx or dy)
STAGES = 20


def sine_cosine(angle):
    half = 0.5 * angle
    w = half * half
    s = jnp.full_like(w, -1.0 / 39916800.0)
    for term in (1.0 / 362880.0, -1.0 / 5040.0, 1.0 / 120.0, -1.0 / 6.0, 1.0):
        s = s * w + term
    s = s * half
    c = jnp.full_like(w, 1.0 / 479001600.0)
    for term in (-1.0 / 3628800.0, 1.0 / 40320.0, -1.0 / 720.0, 1.0 / 24.0, -0.5, 1.0):
        c = c * w + term
    return 2.0 * s * c, 1.0 - 2.0 * s * s


def split(value):
    high = value.astype(BF16)
    return high, (value - high.astype(F32)).astype(BF16)


def times(left, right):
    (lh, ll), (rh, rl) = left, right
    dot = functools.partial(jnp.dot, preferred_element_type=F32)
    return dot(lh, rh) + dot(lh, rl) + dot(ll, rh)


def kernel(amps_in, energies_in, phases_in, mixes_in, out, marg, *scratch):
    (amps, energies, phases, mixes, in_sem, tables, canon, moved, other, e_send, e_mid, e_got, s_buf, s_mid, s_got, t_buf, t_mid, t_oth, t_mix, t_got,
     held, p_send, p_got, p_sum, p_far, send_sem, recv_sem) = scratch
    bank, lane = lax.axis_index("bank"), lax.axis_index("lane")
    x, y, z_hi = bank % 4, (bank // 4) % 4, bank // 16
    z, core = z_hi * 4 + lane // 2, lane % 2
    xy = y * 4 + x

    def z_peer(step):
        there = (z + step) % 8
        return there, ((there // 4) * 16 + xy, (there % 4) * 2 + core)

    def xy_peer(step):
        there = ((y + step[1]) % 4) * 4 + (x + step[0]) % 4
        return there, (z_hi * 16 + there, lane)

    partner = (bank, (lane // 2) * 2 + 1 - core)
    z_peers = [z_peer(step) for step in Z_STEPS]
    xy_peers = [xy_peer(step) for step in XY_STEPS]

    def remote(src, dst, stage, device):
        return pltpu.make_async_remote_copy(
            src_ref=src, dst_ref=dst, send_sem=send_sem.at[stage], recv_sem=recv_sem.at[stage],
            device_id=device, device_id_type=MESH,
        )

    def send_z(src, dst, stage):
        for there, device in z_peers:
            remote(src.at[there], dst.at[z], stage, device).start()
        dst[z] = src[z]

    def send_xy(src, dst, stage, unit):
        for there, device in xy_peers:
            remote(
                src.at[:, pl.ds(pl.multiple_of(there * unit, unit), unit), :],
                dst.at[:, pl.ds(pl.multiple_of(xy * unit, unit), unit), :],
                stage, device,
            ).start()
        own = pl.ds(pl.multiple_of(xy * unit, unit), unit)
        dst[:, own, :] = src[:, own, :]

    def all_of(ref, sem):
        return pltpu.make_async_copy(ref, ref, sem)

    def z_bytes(buf):
        return buf.at[pl.ds(0, 7)]

    def xy_bytes(buf, unit):
        return buf.at[:, pl.ds(0, 15 * unit), :]

    barrier = pltpu.get_barrier_semaphore()
    for _, device in z_peers + xy_peers:
        pl.semaphore_signal(barrier, inc=1, device_id=device, device_id_type=MESH)
    pl.semaphore_signal(barrier, inc=1, device_id=partner, device_id_type=MESH)

    loads = [
        pltpu.make_async_copy(src, dst, in_sem.at[k])
        for k, (src, dst) in enumerate(
            ((energies_in, energies), (mixes_in, mixes), (phases_in, phases), (amps_in, amps))
        )
    ]
    for load in loads:
        load.start()
    loads[0].wait()
    for r0 in range(2):
        for sz in range(8):
            for r1 in range(2):
                e_send[r0, sz, pl.ds(r1, 16, stride=2), :] = energies[
                    sz // 2, pl.ds((sz % 2) * 64 + 2 * r1 + r0, 16, stride=4), :
                ]
    with jax.named_scope("barrier"):
        pl.semaphore_wait(barrier, 23)
    send_z(e_send.at[0], e_mid.at[0], 0)
    send_xy(e_send.at[1], e_mid.at[1], 1, 2)

    for load in loads[1:]:
        load.wait()
    mix_sin, mix_cos = sine_cosine(mixes[...])

    def cs(layer, group, shape):
        at = (slice(layer, layer + 1), slice(group, group + 1))
        return jnp.broadcast_to(mix_cos[at], shape), jnp.broadcast_to(mix_sin[at], shape)

    row = lax.broadcasted_iota(jnp.int32, (128, 128), 0)
    column = lax.broadcasted_iota(jnp.int32, (128, 128), 1)
    apart = row ^ column

    def build(slot, layer, groups, on_left):
        size, count = None, None
        for k, group in enumerate(groups):
            c, s = cs(layer, group, (128, 128))
            bit = (apart >> k) & 1
            factor = jnp.where(bit == 1, s, c)
            size = factor if size is None else size * factor
            count = bit if count is None else count + bit
        odd = (count & 1) == 1
        sign = 1.0 - (count & 2).astype(F32)
        re = jnp.where(odd, 0.0, size * sign)
        im = jnp.where(odd, -size * sign, 0.0)
        for half, (real, imag) in enumerate(zip(split(re), split(im))):
            tables[slot, half, 0:128, 0:128] = real
            tables[slot, half, 128:256, 128:256] = real
            tables[slot, half, 0:128, 128:256] = -imag if on_left else imag
            tables[slot, half, 128:256, 0:128] = imag if on_left else -imag

    def table(slot):
        return tables[slot, 0], tables[slot, 1]

    lanes = (0,) * 7
    rows = (1,) * 5 + (2, 2)
    chips = (2,) * 4 + (3, 3) + (2,)
    build(0, 0, lanes, False)
    build(1, 0, rows, True)

    def turned(re, im, levels, layer):
        angle = jnp.broadcast_to(phases[layer:layer + 1, :], levels.shape) * levels
        s, c = sine_cosine(angle)
        return re * c + im * s, im * c - re * s

    def mixed(u, v, c, s):
        (ur, ui), (vr, vi) = u, v
        return (c * ur + s * vi, c * ui - s * vr), (c * vr + s * ui, c * vi - s * ur)

    shape = (32, 128)
    c1, s1 = cs(0, 1, shape)
    for t in range(4):
        parts = {}
        for q in range(4):
            at = pl.ds(q, 32, stride=4)
            parts[q] = turned(amps[0, t, at, :], amps[1, t, at, :], energies[t, at, :], 0)
        for low, high in ((0, 1), (2, 3), (0, 2), (1, 3)):
            parts[low], parts[high] = mixed(parts[low], parts[high], c1, s1)
        for q in range(4):
            place = ((q % 2) * 2 + q // 2) * 128 + t * 32
            canon[place:place + 32, 0:128] = parts[q][0]
            canon[place:place + 32, 128:256] = parts[q][1]
    for r0 in range(2):
        done = times(split(canon[r0 * 256:r0 * 256 + 256, :]), table(0))
        for r1 in range(2):
            for part in range(2):
                moved[r0, part * 128:part * 128 + 128, r1 * 128:r1 * 128 + 128] = done[
                    r1 * 128:r1 * 128 + 128, part * 128:part * 128 + 128
                ]
        remote(moved.at[r0], other.at[r0], 2 + r0, partner).start()

    def spread(buf, r0, value):
        for sz in range(8):
            for part in range(2):
                for r1 in range(2):
                    buf[r0, sz, pl.ds(2 * part + r1, 16, stride=4), :] = value[
                        part * 128 + sz * 16:part * 128 + sz * 16 + 16, r1 * 128:r1 * 128 + 128
                    ]

    def gathered(buf, r0):
        columns = []
        for r1 in range(2):
            columns.append(jnp.concatenate(
                [buf[r0, sz, pl.ds(2 * part + r1, 16, stride=4), :] for part in range(2) for sz in range(8)], axis=0
            ))
        return jnp.concatenate(columns, axis=1)

    c3, s3 = cs(0, 3, (128, 256))
    for r0 in range(2):
        with jax.named_scope("w" + str(2 + r0)):
            all_of(other.at[r0], recv_sem.at[2 + r0]).wait()
        re = c3 * moved[r0, 0:128, :] + s3 * other[r0, 128:256, :]
        im = c3 * moved[r0, 128:256, :] - s3 * other[r0, 0:128, :]
        spread(s_buf, r0, times(table(1), split(jnp.concatenate([re, im], axis=0))))
        if r0 == 0:
            send_z(s_buf.at[0], s_mid.at[0], 4)
        else:
            send_xy(s_buf.at[1], s_mid.at[1], 5, 4)

    with jax.named_scope("w" + str(0)):
        all_of(z_bytes(e_mid.at[0]), recv_sem.at[0]).wait()
    send_xy(e_mid.at[0], e_got.at[0], 6, 2)
    with jax.named_scope("w" + str(1)):
        all_of(xy_bytes(e_mid.at[1], 2), recv_sem.at[1]).wait()
    send_z(e_mid.at[1], e_got.at[1], 7)

    with jax.named_scope("w" + str(5)):
        all_of(xy_bytes(s_mid.at[1], 4), recv_sem.at[5]).wait()
    send_z(s_mid.at[1], s_got.at[1], 8)
    build(2, 0, chips, True)
    build(3, 1, chips, True)
    with jax.named_scope("w" + str(4)):
        all_of(z_bytes(s_mid.at[0]), recv_sem.at[4]).wait()
    send_xy(s_mid.at[0], s_got.at[0], 9, 4)
    build(4, 1, lanes, False)
    build(5, 1, rows, True)

    def middle(r0):
        value = times(table(2), split(gathered(s_got, r0)))
        c, s = cs(1, 1, (128, 128))
        parts = []
        for r1 in range(2):
            levels = jnp.concatenate([e_got[r0, sz, pl.ds(r1, 16, stride=2), :] for sz in range(8)], axis=0)
            at = slice(r1 * 128, r1 * 128 + 128)
            parts.append(turned(value[0:128, at], value[128:256, at], levels, 1))
        parts = mixed(parts[0], parts[1], c, s)
        value = jnp.concatenate([jnp.concatenate(part, axis=1) for part in parts], axis=0)
        value = times(split(value), table(4))
        value = jnp.concatenate(
            [jnp.concatenate([value[0:128, at], value[128:256, at]], axis=1) for at in (slice(0, 128), slice(128, 256))],
            axis=0,
        )
        held[r0] = times(table(3), split(value))

    with jax.named_scope("w" + str(6)):
        all_of(xy_bytes(e_got.at[0], 2), recv_sem.at[6]).wait()
    with jax.named_scope("w" + str(9)):
        all_of(xy_bytes(s_got.at[0], 4), recv_sem.at[9]).wait()
    middle(0)
    with jax.named_scope("w" + str(7)):
        all_of(z_bytes(e_got.at[1]), recv_sem.at[7]).wait()
    with jax.named_scope("w" + str(8)):
        all_of(z_bytes(s_got.at[1]), recv_sem.at[8]).wait()
    middle(1)

    c0, s0 = cs(1, 1, (128, 256))
    first, second = mixed(
        (held[0, 0:128, :], held[0, 128:256, :]), (held[1, 0:128, :], held[1, 128:256, :]), c0, s0
    )
    spread(t_buf, 1, jnp.concatenate(second, axis=0))
    send_z(t_buf.at[1], t_mid.at[1], 10)
    spread(t_buf, 0, jnp.concatenate(first, axis=0))
    send_xy(t_buf.at[0], t_mid.at[0], 11, 4)

    ck, sk = cs(1, 3, (16, 128))

    def core_mixed(r0):
        for sz in range(8):
            for part in range(2):
                for r1 in range(2):
                    own = t_mid[r0, sz, pl.ds(2 * part + r1, 16, stride=4), :]
                    far = t_oth[r0, sz, pl.ds(2 * (1 - part) + r1, 16, stride=4), :]
                    t_mix[r0, sz, pl.ds(2 * part + r1, 16, stride=4), :] = (
                        ck * own + sk * far if part == 0 else ck * own - sk * far
                    )

    with jax.named_scope("w" + str(11)):
        all_of(xy_bytes(t_mid.at[0], 4), recv_sem.at[11]).wait()
    remote(t_mid.at[0], t_oth.at[0], 12, partner).start()
    with jax.named_scope("w" + str(12)):
        all_of(t_oth.at[0], recv_sem.at[12]).wait()
    core_mixed(0)
    send_z(t_mix.at[0], t_got.at[0], 13)
    with jax.named_scope("w" + str(10)):
        all_of(z_bytes(t_mid.at[1]), recv_sem.at[10]).wait()
    remote(t_mid.at[1], t_oth.at[1], 14, partner).start()
    with jax.named_scope("w" + str(14)):
        all_of(t_oth.at[1], recv_sem.at[14]).wait()
    core_mixed(1)
    send_xy(t_mix.at[1], t_got.at[1], 15, 4)

    def final(r0):
        value = times(table(5), split(gathered(t_got, r0)))
        for part in range(2):
            for t in range(4):
                for r1 in range(2):
                    out[part, t, pl.ds(2 * r1 + r0, 32, stride=4), :] = value[
                        part * 128 + t * 32:part * 128 + t * 32 + 32, r1 * 128:r1 * 128 + 128
                    ]
        chance = value[0:128, :] * value[0:128, :] + value[128:256, :] * value[128:256, :]
        for t in range(4):
            for r6 in range(2):
                for r1 in range(2):
                    at = t * 32 + r6 * 16
                    p_send[r6, pl.ds(t * 4 + r1 * 2 + r0, 16, stride=16), :] = chance[
                        at:at + 16, r1 * 128:r1 * 128 + 128
                    ]

    with jax.named_scope("w" + str(15)):
        all_of(xy_bytes(t_got.at[1], 4), recv_sem.at[15]).wait()
    final(1)
    with jax.named_scope("w" + str(13)):
        all_of(z_bytes(t_got.at[0]), recv_sem.at[13]).wait()
    final(0)

    for there, device in xy_peers:
        remote(
            p_send.at[:, pl.ds(pl.multiple_of(there * 16, 16), 16), :], p_got.at[xy], 16, device
        ).start()
    p_got[xy] = p_send[:, pl.ds(pl.multiple_of(xy * 16, 16), 16), :]
    with jax.named_scope("w" + str(16)):
        all_of(p_got.at[pl.ds(0, 15)], recv_sem.at[16]).wait()
    total = p_got[0]
    for k in range(1, 16):
        total = total + p_got[k]
    p_sum[...] = total
    far = remote(p_sum.at[1 - z_hi], p_far, 17, ((1 - z_hi) * 16 + xy, lane))
    far.start()
    with jax.named_scope("w" + str(17)):
        all_of(p_far, recv_sem.at[17]).wait()
    whole = (p_sum[z_hi] + p_far[...]) * (1.0 / 32.0)
    for t in range(4):
        marg[t] = whole[t * 4:t * 4 + 4, :]

    for stage, buf in (
        (0, z_bytes(e_send.at[0])), (7, z_bytes(e_mid.at[1])), (4, z_bytes(s_buf.at[0])), (8, z_bytes(s_mid.at[1])),
        (10, z_bytes(t_buf.at[1])), (13, z_bytes(t_mix.at[0])),
        (1, xy_bytes(e_send.at[1], 2)), (6, xy_bytes(e_mid.at[0], 2)),
        (5, xy_bytes(s_buf.at[1], 4)), (9, xy_bytes(s_mid.at[0], 4)), (11, xy_bytes(t_buf.at[0], 4)),
        (15, xy_bytes(t_mix.at[1], 4)),
        (2, moved.at[0]), (3, moved.at[1]), (12, t_mid.at[0]), (14, t_mid.at[1]),
        (16, p_got.at[pl.ds(0, 15)]), (17, p_far),
    ):
        all_of(buf, send_sem.at[stage]).wait()


def on_device(amplitudes, energies, phase_angles, mix_angles):
    vmem = pl.BlockSpec(memory_space=pltpu.VMEM)
    half = pltpu.VMEM((2, 8, 64, 128), F32)
    levels = pltpu.VMEM((2, 8, 32, 128), F32)
    wide = pltpu.VMEM((2, 256, 256), F32)
    return pl.pallas_call(
        kernel,
        out_shape=(
            jax.ShapeDtypeStruct((2, 4, 128, 128), F32),
            jax.ShapeDtypeStruct((4, 4, 128), F32),
        ),
        in_specs=[pl.BlockSpec(memory_space=pltpu.HBM)] * 4,
        out_specs=(vmem, vmem),
        scratch_shapes=[
            pltpu.VMEM((2, 4, 128, 128), F32),
            pltpu.VMEM((4, 128, 128), F32),
            pltpu.VMEM((2, 128), F32),
            pltpu.VMEM((2, 4), F32),
            pltpu.SemaphoreType.DMA((4,)),
            pltpu.VMEM((6, 2, 256, 256), BF16),
            pltpu.VMEM((512, 256), F32),
            wide, wide,
            levels, levels, levels,
            half, half, half,
            half, half, half, half, half,
            wide,
            pltpu.VMEM((2, 256, 128), F32),
            pltpu.VMEM((16, 2, 16, 128), F32),
            pltpu.VMEM((2, 16, 128), F32),
            pltpu.VMEM((16, 128), F32),
            pltpu.SemaphoreType.DMA((STAGES,)),
            pltpu.SemaphoreType.DMA((STAGES,)),
        ],
        compiler_params=pltpu.CompilerParams(
            collective_id=0, has_side_effects=True, vmem_limit_bytes=48 * 1024 * 1024
        ),
    )(*[pltpu.with_memory_space_constraint(a, pltpu.HBM) for a in (amplitudes, energies, phase_angles, mix_angles)])


def solution(mesh):
    placed = (P(None, ("bank", "lane"), None, None), P(("bank", "lane"), None, None), P(), P())
    return jax.shard_map(
        on_device,
        mesh=mesh,
        in_specs=placed,
        out_specs=(P(None, ("bank", "lane"), None, None), P("lane", "bank", None)),
        check_vma=False,
    )
```

```python
import functools

import jax
import jax.numpy as jnp
from jax import lax
from jax.experimental import pallas as pl
from jax.experimental.pallas import tpu as pltpu
from jax.sharding import PartitionSpec as P

MESH = pl.DeviceIdType.MESH
F32 = jnp.float32
BF16 = jnp.bfloat16

Z_STEPS = (4, 3, 5, 2, 6, 1, 7)
XY_STEPS = tuple((dx, dy) for dx in (2, 1, 3, 0) for dy in (2, 1, 3, 0) if dx or dy)
ORDER = (0, 2, 1, 3)
Z_FIRST, XY_FIRST = (0, 1), (2, 3)
STAGES = 34


def sine_cosine(angle):
    half = 0.5 * angle
    w = half * half
    s = jnp.full_like(w, -1.0 / 39916800.0)
    for term in (1.0 / 362880.0, -1.0 / 5040.0, 1.0 / 120.0, -1.0 / 6.0, 1.0):
        s = s * w + term
    s = s * half
    c = jnp.full_like(w, 1.0 / 479001600.0)
    for term in (-1.0 / 3628800.0, 1.0 / 40320.0, -1.0 / 720.0, 1.0 / 24.0, -0.5, 1.0):
        c = c * w + term
    return 2.0 * s * c, 1.0 - 2.0 * s * s


def split(value):
    high = value.astype(BF16)
    return high, (value - high.astype(F32)).astype(BF16)


def times(left, right):
    (lh, ll), (rh, rl) = left, right
    dot = functools.partial(jnp.dot, preferred_element_type=F32)
    return dot(lh, rh) + dot(lh, rl) + dot(ll, rh)


def kernel(amps_in, energies_in, phases_in, mixes_in, out, marg, *scratch):
    (amps, energies, phases, mixes, in_sem, tables, canon, moved, other, e_send, e_mid, e_got, s_buf, s_mid, s_got,
     held, held_far, t_buf, t_mid, t_got, last, p_send, p_got, p_sum, p_far, send_sem, recv_sem) = scratch
    bank, lane = lax.axis_index("bank"), lax.axis_index("lane")
    x, y, z_hi = bank % 4, (bank // 4) % 4, bank // 16
    z, core = z_hi * 4 + lane // 2, lane % 2
    xy = y * 4 + x

    def z_peer(step):
        there = (z + step) % 8
        return there, ((there // 4) * 16 + xy, (there % 4) * 2 + core)

    def xy_peer(step):
        there = ((y + step[1]) % 4) * 4 + (x + step[0]) % 4
        return there, (z_hi * 16 + there, lane)

    partner = (bank, (lane // 2) * 2 + 1 - core)
    z_peers = [z_peer(step) for step in Z_STEPS]
    xy_peers = [xy_peer(step) for step in XY_STEPS]

    barrier = pltpu.get_barrier_semaphore()
    for _, device in z_peers + xy_peers:
        pl.semaphore_signal(barrier, inc=1, device_id=device, device_id_type=MESH)
    pl.semaphore_signal(barrier, inc=1, device_id=partner, device_id_type=MESH)
    loads = [
        pltpu.make_async_copy(src, dst, in_sem.at[k])
        for k, (src, dst) in enumerate(
            ((energies_in, energies), (mixes_in, mixes), (phases_in, phases), (amps_in, amps))
        )
    ]
    for load in loads:
        load.start()

    sent = []

    def remote(src, dst, stage, device):
        return pltpu.make_async_remote_copy(
            src_ref=src, dst_ref=dst, send_sem=send_sem.at[stage], recv_sem=recv_sem.at[stage],
            device_id=device, device_id_type=MESH,
        )

    def all_of(ref, sem):
        return pltpu.make_async_copy(ref, ref, sem)

    def arrived(ref, stage):
        with jax.named_scope(f"w{stage}"):
            all_of(ref, recv_sem.at[stage]).wait()

    def send_z(src, dst, stage):
        for there, device in z_peers:
            remote(src.at[there], dst.at[z], stage, device).start()
        dst[z] = src[z]
        sent.append((src.at[pl.ds(0, 7)], stage))

    def send_xy(src, dst, stage, unit):
        own = pl.ds(xy * unit, unit)
        for there, device in xy_peers:
            remote(src.at[:, pl.ds(there * unit, unit), :], dst.at[:, own, :], stage, device).start()
        dst[:, own, :] = src[:, own, :]
        sent.append((src.at[:, pl.ds(0, 15 * unit), :], stage))

    def swap(src, dst, stage):
        remote(src, dst, stage, partner).start()
        sent.append((src, stage))

    def came_z(buf, stage):
        arrived(buf.at[pl.ds(0, 7)], stage)

    def came_xy(buf, stage, unit):
        arrived(buf.at[:, pl.ds(0, 15 * unit), :], stage)

    E1, E2, S1, S2, D1, D2, T1, T2, P1, P2 = 0, 4, 8, 12, 16, 20, 24, 28, 32, 33

    loads[0].wait()
    for q in range(4):
        for sz in range(8):
            e_send[q, sz] = energies[sz // 2, pl.ds((sz % 2) * 64 + q, 16, stride=4), :]
    with jax.named_scope("barrier"):
        pl.semaphore_wait(barrier, 23)
    for q in Z_FIRST:
        send_z(e_send.at[q], e_mid.at[q], E1 + q)
    for q in XY_FIRST:
        send_xy(e_send.at[q], e_mid.at[q], E1 + q, 1)

    for load in loads[1:]:
        load.wait()
    mix_sin, mix_cos = sine_cosine(mixes[...])

    def cs(layer, group, shape):
        at = (slice(layer, layer + 1), slice(group, group + 1))
        return jnp.broadcast_to(mix_cos[at], shape), jnp.broadcast_to(mix_sin[at], shape)

    row = lax.broadcasted_iota(jnp.int32, (128, 128), 0)
    column = lax.broadcasted_iota(jnp.int32, (128, 128), 1)
    apart = row ^ column

    def build(slot, layer, groups, on_left):
        size, count = None, None
        for k, group in enumerate(groups):
            c, s = cs(layer, group, (128, 128))
            bit = (apart >> k) & 1
            factor = jnp.where(bit == 1, s, c)
            size = factor if size is None else size * factor
            count = bit if count is None else count + bit
        odd = (count & 1) == 1
        sign = 1.0 - (count & 2).astype(F32)
        re = jnp.where(odd, 0.0, size * sign)
        im = jnp.where(odd, -size * sign, 0.0)
        for half, (real, imag) in enumerate(zip(split(re), split(im))):
            tables[slot, half, 0:128, 0:128] = real
            tables[slot, half, 128:256, 128:256] = real
            tables[slot, half, 0:128, 128:256] = -imag if on_left else imag
            tables[slot, half, 128:256, 0:128] = imag if on_left else -imag

    def table(slot):
        return tables[slot, 0], tables[slot, 1]

    lanes = (0,) * 7
    rows = (1,) * 5 + (2, 2)
    chips = (2,) * 4 + (3, 3) + (2,)
    build(0, 0, lanes, False)
    build(1, 0, rows, True)

    def turned(re, im, levels, layer):
        angle = jnp.broadcast_to(phases[layer:layer + 1, :], levels.shape) * levels
        s, c = sine_cosine(angle)
        return re * c + im * s, im * c - re * s

    def mixed(u, v, c, s):
        (ur, ui), (vr, vi) = u, v
        return (c * ur + s * vi, c * ui - s * vr), (c * vr + s * ui, c * vi - s * ur)

    c1, s1 = cs(0, 1, (32, 128))
    for t in range(4):
        parts = {}
        for q in range(4):
            at = pl.ds(q, 32, stride=4)
            parts[q] = turned(amps[0, t, at, :], amps[1, t, at, :], energies[t, at, :], 0)
        for low, high in ((0, 1), (2, 3), (0, 2), (1, 3)):
            parts[low], parts[high] = mixed(parts[low], parts[high], c1, s1)
        for q in range(4):
            for part in range(2):
                canon[q, t * 32:t * 32 + 32, part * 128:part * 128 + 128] = parts[q][part]
    for q in ORDER:
        done = times(split(canon[q]), table(0))
        moved[q, 0:128, :] = done[:, 0:128]
        moved[q, 128:256, :] = done[:, 128:256]
        swap(moved.at[q], other.at[q], D1 + q)

    def core_mixed(near, far, q, layer):
        c, s = cs(layer, 3, (128, 128))
        re = c * near[q, 0:128, :] + s * far[q, 128:256, :]
        im = c * near[q, 128:256, :] - s * far[q, 0:128, :]
        return jnp.concatenate([re, im], axis=0)

    def spread(buf, q, value):
        for sz in range(8):
            for part in range(2):
                at = part * 128 + sz * 16
                buf[q, sz, pl.ds(part, 16, stride=2), :] = value[at:at + 16, :]

    def gathered(buf, q):
        return jnp.concatenate(
            [buf[q, sz, pl.ds(part, 16, stride=2), :] for part in range(2) for sz in range(8)], axis=0
        )

    for q in ORDER:
        arrived(other.at[q], D1 + q)
        spread(s_buf, q, times(table(1), split(core_mixed(moved, other, q, 0))))
        if q in Z_FIRST:
            send_z(s_buf.at[q], s_mid.at[q], S1 + q)
        else:
            send_xy(s_buf.at[q], s_mid.at[q], S1 + q, 2)
    build(2, 0, chips, True)

    for q in XY_FIRST:
        came_xy(e_mid.at[q], E1 + q, 1)
        send_z(e_mid.at[q], e_got.at[q], E2 + q)
    for q in Z_FIRST:
        came_z(e_mid.at[q], E1 + q)
        send_xy(e_mid.at[q], e_got.at[q], E2 + q, 1)
    build(3, 1, chips, True)
    build(4, 1, lanes, False)
    build(5, 1, rows, True)

    def forward(q):
        if q in Z_FIRST:
            came_z(s_mid.at[q], S1 + q)
            send_xy(s_mid.at[q], s_got.at[q], S2 + q, 2)
        else:
            came_xy(s_mid.at[q], S1 + q, 2)
            send_z(s_mid.at[q], s_got.at[q], S2 + q)

    def middle(q):
        if q in Z_FIRST:
            came_xy(e_got.at[q], E2 + q, 1)
            came_xy(s_got.at[q], S2 + q, 2)
        else:
            came_z(e_got.at[q], E2 + q)
            came_z(s_got.at[q], S2 + q)
        value = times(table(2), split(gathered(s_got, q)))
        levels = jnp.concatenate([e_got[q, sz] for sz in range(8)], axis=0)
        value = jnp.concatenate(turned(value[0:128, :], value[128:256, :], levels, 1), axis=1)
        value = times(split(value), table(4))
        value = jnp.concatenate([value[:, 0:128], value[:, 128:256]], axis=0)
        held[q] = times(table(3), split(value))
        swap(held.at[q], held_far.at[q], D2 + q)

    def back(q):
        arrived(held_far.at[q], D2 + q)
        spread(t_buf, q, core_mixed(held, held_far, q, 1))
        if q in Z_FIRST:
            send_z(t_buf.at[q], t_mid.at[q], T1 + q)
        else:
            send_xy(t_buf.at[q], t_mid.at[q], T1 + q, 2)

    def home(q):
        if q in Z_FIRST:
            came_z(t_mid.at[q], T1 + q)
            send_xy(t_mid.at[q], t_got.at[q], T2 + q, 2)
        else:
            came_xy(t_mid.at[q], T1 + q, 2)
            send_z(t_mid.at[q], t_got.at[q], T2 + q)

    def final(q):
        if q in Z_FIRST:
            came_xy(t_got.at[q], T2 + q, 2)
        else:
            came_z(t_got.at[q], T2 + q)
        last[q] = times(table(5), split(gathered(t_got, q)))

    cr, sr = cs(1, 1, (128, 128))

    def pair(low, high):
        first, second = mixed(
            (last[low, 0:128, :], last[low, 128:256, :]), (last[high, 0:128, :], last[high, 128:256, :]), cr, sr
        )
        for q, value in ((low, first), (high, second)):
            last[q, 0:128, :], last[q, 128:256, :] = value

    forward(0)
    forward(2)
    forward(3)
    forward(1)
    middle(0)
    back(0)
    middle(1)
    middle(2)
    back(1)
    back(2)
    middle(3)
    back(3)
    home(0)
    home(2)
    home(1)
    home(3)
    final(0)
    final(2)
    pair(0, 2)
    final(1)
    final(3)
    pair(1, 3)
    pair(0, 1)
    pair(2, 3)

    for q in range(4):
        chance = last[q, 0:128, :] * last[q, 0:128, :] + last[q, 128:256, :] * last[q, 128:256, :]
        for t in range(4):
            for r6 in range(2):
                at = t * 32 + r6 * 16
                p_send[r6, pl.ds(t * 4 + q, 16, stride=16), :] = chance[at:at + 16, :]
    for there, device in xy_peers:
        remote(p_send.at[:, pl.ds(pl.multiple_of(there * 16, 16), 16), :], p_got.at[xy], P1, device).start()
    p_got[xy] = p_send[:, pl.ds(pl.multiple_of(xy * 16, 16), 16), :]
    for q in range(4):
        for part in range(2):
            for t in range(4):
                at = part * 128 + t * 32
                out[part, t, pl.ds(q, 32, stride=4), :] = last[q, at:at + 32, :]
    arrived(p_got.at[pl.ds(0, 15)], P1)
    total = p_got[0]
    for k in range(1, 16):
        total = total + p_got[k]
    p_sum[...] = total
    remote(p_sum.at[1 - z_hi], p_far, P2, ((1 - z_hi) * 16 + xy, lane)).start()
    sent.append((p_got.at[pl.ds(0, 15)], P1))
    for buf, stage in sent:
        all_of(buf, send_sem.at[stage]).wait()
    arrived(p_far, P2)
    whole = (p_sum[z_hi] + p_far[...]) * (1.0 / 32.0)
    for t in range(4):
        marg[t] = whole[t * 4:t * 4 + 4, :]
    all_of(p_far, send_sem.at[P2]).wait()


def on_device(amplitudes, energies, phase_angles, mix_angles):
    vmem = pl.BlockSpec(memory_space=pltpu.VMEM)
    state = pltpu.VMEM((4, 8, 32, 128), F32)
    levels = pltpu.VMEM((4, 8, 16, 128), F32)
    tall = pltpu.VMEM((4, 256, 128), F32)
    return pl.pallas_call(
        kernel,
        out_shape=(
            jax.ShapeDtypeStruct((2, 4, 128, 128), F32),
            jax.ShapeDtypeStruct((4, 4, 128), F32),
        ),
        in_specs=[pl.BlockSpec(memory_space=pltpu.HBM)] * 4,
        out_specs=(vmem, vmem),
        scratch_shapes=[
            pltpu.VMEM((2, 4, 128, 128), F32),
            pltpu.VMEM((4, 128, 128), F32),
            pltpu.VMEM((2, 128), F32),
            pltpu.VMEM((2, 4), F32),
            pltpu.SemaphoreType.DMA((4,)),
            pltpu.VMEM((6, 2, 256, 256), BF16),
            pltpu.VMEM((4, 128, 256), F32),
            tall, tall,
            levels, levels, levels,
            state, state, state,
            tall, tall,
            state, state, state,
            tall,
            pltpu.VMEM((2, 256, 128), F32),
            pltpu.VMEM((16, 2, 16, 128), F32),
            pltpu.VMEM((2, 16, 128), F32),
            pltpu.VMEM((16, 128), F32),
            pltpu.SemaphoreType.DMA((STAGES,)),
            pltpu.SemaphoreType.DMA((STAGES,)),
        ],
        compiler_params=pltpu.CompilerParams(
            collective_id=0, has_side_effects=True, vmem_limit_bytes=48 * 1024 * 1024
        ),
    )(*[pltpu.with_memory_space_constraint(a, pltpu.HBM) for a in (amplitudes, energies, phase_angles, mix_angles)])


def solution(mesh):
    placed = (P(None, ("bank", "lane"), None, None), P(("bank", "lane"), None, None), P(), P())
    return jax.shard_map(
        on_device,
        mesh=mesh,
        in_specs=placed,
        out_specs=(P(None, ("bank", "lane"), None, None), P("lane", "bank", None)),
        check_vma=False,
    )
```

```python
import functools

import jax
import jax.numpy as jnp
from jax import lax
from jax.experimental import pallas as pl
from jax.experimental.pallas import tpu as pltpu
from jax.sharding import PartitionSpec as P

MESH = pl.DeviceIdType.MESH
F32 = jnp.float32
BF16 = jnp.bfloat16

Z_STEPS = (4, 3, 5, 2, 6, 1, 7)
XY_STEPS = ((2, 2), (1, 2), (3, 2), (0, 2), (2, 1), (2, 3), (1, 1), (3, 3), (0, 1), (0, 3), (1, 3), (3, 1), (2, 0), (1, 0), (3, 0))
ORDER = (0, 2, 1, 3)
Z_FIRST, XY_FIRST = (0, 1), (2, 3)
STAGES = 35


def sine_cosine(angle):
    half = 0.5 * angle
    w = half * half
    s = jnp.full_like(w, -1.0 / 39916800.0)
    for term in (1.0 / 362880.0, -1.0 / 5040.0, 1.0 / 120.0, -1.0 / 6.0, 1.0):
        s = s * w + term
    s = s * half
    c = jnp.full_like(w, 1.0 / 479001600.0)
    for term in (-1.0 / 3628800.0, 1.0 / 40320.0, -1.0 / 720.0, 1.0 / 24.0, -0.5, 1.0):
        c = c * w + term
    return 2.0 * s * c, 1.0 - 2.0 * s * s


def split(value):
    high = value.astype(BF16)
    return high, (value - high.astype(F32)).astype(BF16)


def times(left, right):
    (lh, ll), (rh, rl) = left, right
    dot = functools.partial(jnp.dot, preferred_element_type=F32)
    return dot(lh, rh) + dot(lh, rl) + dot(ll, rh)


def kernel(amps_in, energies_in, phases_in, mixes_in, out, marg, *scratch):
    (amps, energies, phases, mixes, in_sem, tables, canon, moved, other, e_send, e_mid, e_got, s_buf, s_mid, s_got,
     held, held_far, t_buf, t_mid, t_got, last, p_send, p_got, p_sum, p_far, send_sem, recv_sem) = scratch
    bank, lane = lax.axis_index("bank"), lax.axis_index("lane")
    x, y, z_hi = bank % 4, (bank // 4) % 4, bank // 16
    z, core = z_hi * 4 + lane // 2, lane % 2
    xy = y * 4 + x

    def z_peer(step):
        there = (z + step) % 8
        return there, ((there // 4) * 16 + xy, (there % 4) * 2 + core)

    def xy_peer(step):
        there = ((y + step[1]) % 4) * 4 + (x + step[0]) % 4
        return there, (z_hi * 16 + there, lane)

    partner = (bank, (lane // 2) * 2 + 1 - core)
    z_peers = [z_peer(step) for step in Z_STEPS]
    xy_peers = [xy_peer(step) for step in XY_STEPS]

    barrier = pltpu.get_barrier_semaphore()
    for _, device in z_peers + xy_peers:
        pl.semaphore_signal(barrier, inc=1, device_id=device, device_id_type=MESH)
    pl.semaphore_signal(barrier, inc=1, device_id=partner, device_id_type=MESH)
    loads = [
        pltpu.make_async_copy(src, dst, in_sem.at[k])
        for k, (src, dst) in enumerate(
            ((energies_in, energies), (mixes_in, mixes), (phases_in, phases), (amps_in, amps))
        )
    ]
    for load in loads:
        load.start()

    sent = []

    def remote(src, dst, stage, device):
        return pltpu.make_async_remote_copy(
            src_ref=src, dst_ref=dst, send_sem=send_sem.at[stage], recv_sem=recv_sem.at[stage],
            device_id=device, device_id_type=MESH,
        )

    def all_of(ref, sem):
        return pltpu.make_async_copy(ref, ref, sem)

    def arrived(ref, stage):
        with jax.named_scope(f"w{stage}"):
            all_of(ref, recv_sem.at[stage]).wait()

    def send_z(src, dst, stage):
        for there, device in z_peers:
            remote(src.at[there], dst.at[z], stage, device).start()
        dst[z] = src[z]
        sent.append((src.at[pl.ds(0, 7)], stage))

    def send_xy(src, dst, stage, unit):
        own = pl.ds(xy * unit, unit)
        for there, device in xy_peers:
            remote(src.at[:, pl.ds(there * unit, unit), :], dst.at[:, own, :], stage, device).start()
        dst[:, own, :] = src[:, own, :]
        sent.append((src.at[:, pl.ds(0, 15 * unit), :], stage))

    def swap(src, dst, stage):
        remote(src, dst, stage, partner).start()
        sent.append((src, stage))

    def came_z(buf, stage):
        arrived(buf.at[pl.ds(0, 7)], stage)

    def came_xy(buf, stage, unit):
        arrived(buf.at[:, pl.ds(0, 15 * unit), :], stage)

    E1, E2, S1, S2, D1, D2, T1, T2, P1, P2 = 0, 4, 8, 12, 16, 20, 24, 28, 32, 34

    loads[0].wait()
    for q in range(4):
        for sz in range(8):
            e_send[q, sz] = energies[sz // 2, pl.ds((sz % 2) * 64 + q, 16, stride=4), :]
    with jax.named_scope("barrier"):
        pl.semaphore_wait(barrier, 23)
    for q in Z_FIRST:
        send_z(e_send.at[q], e_mid.at[q], E1 + q)
    for q in XY_FIRST:
        send_xy(e_send.at[q], e_mid.at[q], E1 + q, 1)

    for load in loads[1:]:
        load.wait()
    mix_sin, mix_cos = sine_cosine(mixes[...])

    def cs(layer, group, shape):
        at = (slice(layer, layer + 1), slice(group, group + 1))
        return jnp.broadcast_to(mix_cos[at], shape), jnp.broadcast_to(mix_sin[at], shape)

    row = lax.broadcasted_iota(jnp.int32, (128, 128), 0)
    column = lax.broadcasted_iota(jnp.int32, (128, 128), 1)
    apart = row ^ column

    def build(slot, layer, groups, on_left):
        size, count = None, None
        for k, group in enumerate(groups):
            c, s = cs(layer, group, (128, 128))
            bit = (apart >> k) & 1
            factor = jnp.where(bit == 1, s, c)
            size = factor if size is None else size * factor
            count = bit if count is None else count + bit
        odd = (count & 1) == 1
        sign = 1.0 - (count & 2).astype(F32)
        re = jnp.where(odd, 0.0, size * sign)
        im = jnp.where(odd, -size * sign, 0.0)
        for half, (real, imag) in enumerate(zip(split(re), split(im))):
            tables[slot, half, 0:128, 0:128] = real
            tables[slot, half, 128:256, 128:256] = real
            tables[slot, half, 0:128, 128:256] = -imag if on_left else imag
            tables[slot, half, 128:256, 0:128] = imag if on_left else -imag

    def table(slot):
        return tables[slot, 0], tables[slot, 1]

    lanes = (0,) * 7
    rows = (1,) * 5 + (2, 2)
    chips = (2,) * 4 + (3, 3) + (2,)
    build(0, 0, lanes, False)
    build(1, 0, rows, True)

    def turned(re, im, levels, layer):
        angle = jnp.broadcast_to(phases[layer:layer + 1, :], levels.shape) * levels
        s, c = sine_cosine(angle)
        return re * c + im * s, im * c - re * s

    def mixed(u, v, c, s):
        (ur, ui), (vr, vi) = u, v
        return (c * ur + s * vi, c * ui - s * vr), (c * vr + s * ui, c * vi - s * ur)

    c1, s1 = cs(0, 1, (32, 128))
    for t in range(4):
        parts = {}
        for q in range(4):
            at = pl.ds(q, 32, stride=4)
            parts[q] = turned(amps[0, t, at, :], amps[1, t, at, :], energies[t, at, :], 0)
        for low, high in ((0, 1), (2, 3), (0, 2), (1, 3)):
            parts[low], parts[high] = mixed(parts[low], parts[high], c1, s1)
        for q in range(4):
            for part in range(2):
                canon[q, t * 32:t * 32 + 32, part * 128:part * 128 + 128] = parts[q][part]
    for q in ORDER:
        done = times(split(canon[q]), table(0))
        moved[q, 0:128, :] = done[:, 0:128]
        moved[q, 128:256, :] = done[:, 128:256]
        swap(moved.at[q], other.at[q], D1 + q)

    def core_mixed(near, far, q, layer):
        c, s = cs(layer, 3, (128, 128))
        re = c * near[q, 0:128, :] + s * far[q, 128:256, :]
        im = c * near[q, 128:256, :] - s * far[q, 0:128, :]
        return jnp.concatenate([re, im], axis=0)

    def spread(buf, q, value):
        for sz in range(8):
            for part in range(2):
                at = part * 128 + sz * 16
                buf[q, sz, pl.ds(part, 16, stride=2), :] = value[at:at + 16, :]

    def gathered(buf, q):
        return jnp.concatenate(
            [buf[q, sz, pl.ds(part, 16, stride=2), :] for part in range(2) for sz in range(8)], axis=0
        )

    for q in ORDER:
        arrived(other.at[q], D1 + q)
        spread(s_buf, q, times(table(1), split(core_mixed(moved, other, q, 0))))
        if q in Z_FIRST:
            send_z(s_buf.at[q], s_mid.at[q], S1 + q)
        else:
            send_xy(s_buf.at[q], s_mid.at[q], S1 + q, 2)
    build(2, 0, chips, True)

    for q in XY_FIRST:
        came_xy(e_mid.at[q], E1 + q, 1)
        send_z(e_mid.at[q], e_got.at[q], E2 + q)
    for q in Z_FIRST:
        came_z(e_mid.at[q], E1 + q)
        send_xy(e_mid.at[q], e_got.at[q], E2 + q, 1)
    build(3, 1, chips, True)
    build(4, 1, lanes, False)
    build(5, 1, rows, True)

    def forward(q):
        if q in Z_FIRST:
            came_z(s_mid.at[q], S1 + q)
            send_xy(s_mid.at[q], s_got.at[q], S2 + q, 2)
        else:
            came_xy(s_mid.at[q], S1 + q, 2)
            send_z(s_mid.at[q], s_got.at[q], S2 + q)

    def middle(q):
        if q in Z_FIRST:
            came_xy(e_got.at[q], E2 + q, 1)
            came_xy(s_got.at[q], S2 + q, 2)
        else:
            came_z(e_got.at[q], E2 + q)
            came_z(s_got.at[q], S2 + q)
        value = times(table(2), split(gathered(s_got, q)))
        levels = jnp.concatenate([e_got[q, sz] for sz in range(8)], axis=0)
        value = jnp.concatenate(turned(value[0:128, :], value[128:256, :], levels, 1), axis=1)
        value = times(split(value), table(4))
        value = jnp.concatenate([value[:, 0:128], value[:, 128:256]], axis=0)
        held[q] = times(table(3), split(value))
        swap(held.at[q], held_far.at[q], D2 + q)

    def back(q):
        arrived(held_far.at[q], D2 + q)
        spread(t_buf, q, core_mixed(held, held_far, q, 1))
        if q in Z_FIRST:
            send_z(t_buf.at[q], t_mid.at[q], T1 + q)
        else:
            send_xy(t_buf.at[q], t_mid.at[q], T1 + q, 2)

    def home(q):
        if q in Z_FIRST:
            came_z(t_mid.at[q], T1 + q)
            send_xy(t_mid.at[q], t_got.at[q], T2 + q, 2)
        else:
            came_xy(t_mid.at[q], T1 + q, 2)
            send_z(t_mid.at[q], t_got.at[q], T2 + q)

    def final(q):
        if q in Z_FIRST:
            came_xy(t_got.at[q], T2 + q, 2)
        else:
            came_z(t_got.at[q], T2 + q)
        last[q] = times(table(5), split(gathered(t_got, q)))

    cr, sr = cs(1, 1, (128, 128))

    def pair(low, high):
        first, second = mixed(
            (last[low, 0:128, :], last[low, 128:256, :]), (last[high, 0:128, :], last[high, 128:256, :]), cr, sr
        )
        for q, value in ((low, first), (high, second)):
            last[q, 0:128, :], last[q, 128:256, :] = value

    forward(0)
    forward(2)
    forward(3)
    forward(1)
    middle(0)
    back(0)
    middle(1)
    middle(2)
    back(1)
    back(2)
    middle(3)
    back(3)
    home(0)
    home(2)
    home(1)
    home(3)
    final(0)
    final(2)
    pair(0, 2)
    final(1)
    final(3)
    pair(1, 3)
    pair(0, 1)
    pair(2, 3)

    for q in range(4):
        chance = last[q, 0:128, :] * last[q, 0:128, :] + last[q, 128:256, :] * last[q, 128:256, :]
        for t in range(4):
            for r6 in range(2):
                at = t * 32 + r6 * 16
                p_send[r6, pl.ds(t * 4 + q, 16, stride=16), :] = chance[at:at + 16, :]
    for half, stage in ((1 - z_hi, P1), (z_hi, P1 + 1)):
        for there, device in xy_peers:
            remote(
                p_send.at[half, pl.ds(pl.multiple_of(there * 16, 16), 16), :], p_got.at[stage - P1, xy], stage, device
            ).start()
        p_got[stage - P1, xy] = p_send[half, pl.ds(pl.multiple_of(xy * 16, 16), 16), :]
        sent.append((p_got.at[stage - P1, pl.ds(0, 15)], stage))
    for q in range(4):
        for part in range(2):
            for t in range(4):
                at = part * 128 + t * 32
                out[part, t, pl.ds(q, 32, stride=4), :] = last[q, at:at + 32, :]

    def summed(half):
        arrived(p_got.at[half, pl.ds(0, 15)], P1 + half)
        parts = [p_got[half, k] for k in range(16)]
        while len(parts) > 1:
            parts = [parts[k] + parts[k + 1] for k in range(0, len(parts), 2)]
        return parts[0]

    p_sum[...] = summed(0)
    remote(p_sum, p_far, P2, ((1 - z_hi) * 16 + xy, lane)).start()
    near = summed(1)
    for buf, stage in sent:
        all_of(buf, send_sem.at[stage]).wait()
    arrived(p_far, P2)
    marg[...] = (near + p_far[...]) * (1.0 / 32.0)
    all_of(p_far, send_sem.at[P2]).wait()


def writer(parts, chance, parts_out, chance_out, staged, sem):
    copies = [pltpu.make_async_copy(parts, parts_out, sem.at[0]), pltpu.make_async_copy(staged, chance_out, sem.at[1])]
    copies[0].start()
    for t in range(4):
        staged[t] = chance[t * 4:t * 4 + 4, :]
    copies[1].start()
    for copy in copies:
        copy.wait()


def on_device(amplitudes, energies, phase_angles, mix_angles):
    vmem = pl.BlockSpec(memory_space=pltpu.VMEM)
    state = pltpu.VMEM((4, 8, 32, 128), F32)
    levels = pltpu.VMEM((4, 8, 16, 128), F32)
    tall = pltpu.VMEM((4, 256, 128), F32)
    parts, chance = pl.pallas_call(
        kernel,
        out_shape=(
            jax.ShapeDtypeStruct((2, 4, 128, 128), F32),
            jax.ShapeDtypeStruct((16, 128), F32),
        ),
        in_specs=[pl.BlockSpec(memory_space=pltpu.HBM)] * 4,
        out_specs=(vmem, vmem),
        scratch_shapes=[
            pltpu.VMEM((2, 4, 128, 128), F32),
            pltpu.VMEM((4, 128, 128), F32),
            pltpu.VMEM((2, 128), F32),
            pltpu.VMEM((2, 4), F32),
            pltpu.SemaphoreType.DMA((4,)),
            pltpu.VMEM((6, 2, 256, 256), BF16),
            pltpu.VMEM((4, 128, 256), F32),
            tall, tall,
            levels, levels, levels,
            state, state, state,
            tall, tall,
            state, state, state,
            tall,
            pltpu.VMEM((2, 256, 128), F32),
            pltpu.VMEM((2, 16, 16, 128), F32),
            pltpu.VMEM((16, 128), F32),
            pltpu.VMEM((16, 128), F32),
            pltpu.SemaphoreType.DMA((STAGES,)),
            pltpu.SemaphoreType.DMA((STAGES,)),
        ],
        compiler_params=pltpu.CompilerParams(
            collective_id=0, has_side_effects=True, vmem_limit_bytes=48 * 1024 * 1024
        ),
    )(*[pltpu.with_memory_space_constraint(a, pltpu.HBM) for a in (amplitudes, energies, phase_angles, mix_angles)])
    hbm = pl.BlockSpec(memory_space=pltpu.HBM)
    return pl.pallas_call(
        writer,
        out_shape=(
            jax.ShapeDtypeStruct((2, 4, 128, 128), F32),
            jax.ShapeDtypeStruct((4, 4, 128), F32),
        ),
        in_specs=[vmem] * 2,
        out_specs=(hbm, hbm),
        scratch_shapes=[pltpu.VMEM((4, 4, 128), F32), pltpu.SemaphoreType.DMA((2,))],
        compiler_params=pltpu.CompilerParams(vmem_limit_bytes=1024 * 1024),
    )(parts, chance)


def solution(mesh):
    placed = (P(None, ("bank", "lane"), None, None), P(("bank", "lane"), None, None), P(), P())
    return jax.shard_map(
        on_device,
        mesh=mesh,
        in_specs=placed,
        out_specs=(P(None, ("bank", "lane"), None, None), P("lane", "bank", None)),
        check_vma=False,
    )
```

```python
import functools

import jax
import jax.numpy as jnp
from jax import lax
from jax.experimental import pallas as pl
from jax.experimental.pallas import tpu as pltpu
from jax.sharding import PartitionSpec as P

MESH = pl.DeviceIdType.MESH
F32 = jnp.float32
BF16 = jnp.bfloat16

Z_STEPS = (4, 3, 5, 2, 6, 1, 7)
XY_STEPS = ((2, 2), (1, 2), (3, 2), (0, 2), (2, 1), (2, 3), (1, 1), (3, 3), (0, 1), (0, 3), (1, 3), (3, 1), (2, 0), (1, 0), (3, 0))
ORDER = (0, 2, 1, 3)
Z_FIRST, XY_FIRST = (0, 1), (2, 3)
STAGES = 35


def sine_cosine(angle):
    half = 0.5 * angle
    w = half * half
    s = jnp.full_like(w, -1.0 / 39916800.0)
    for term in (1.0 / 362880.0, -1.0 / 5040.0, 1.0 / 120.0, -1.0 / 6.0, 1.0):
        s = s * w + term
    s = s * half
    c = jnp.full_like(w, 1.0 / 479001600.0)
    for term in (-1.0 / 3628800.0, 1.0 / 40320.0, -1.0 / 720.0, 1.0 / 24.0, -0.5, 1.0):
        c = c * w + term
    return 2.0 * s * c, 1.0 - 2.0 * s * s


def split(value):
    high = value.astype(BF16)
    return high, (value - high.astype(F32)).astype(BF16)


def times(left, right):
    (lh, ll), (rh, rl) = left, right
    dot = functools.partial(jnp.dot, preferred_element_type=F32)
    columns = rh.shape[1]
    both = dot(lh, jnp.concatenate([rh, rl], axis=1))
    return both[:, 0:columns] + both[:, columns:] + dot(ll, rh)


def kernel(amps_in, energies_in, phases_in, mixes_in, out, marg, *scratch):
    (amps, energies, phases, mixes, in_sem, tables, canon, moved, other, e_send, e_mid, e_got, s_buf, s_mid, s_got,
     held, held_far, t_buf, t_mid, t_got, last, p_send, p_got, p_sum, p_far, send_sem, recv_sem) = scratch
    bank, lane = lax.axis_index("bank"), lax.axis_index("lane")
    x, y, z_hi = bank % 4, (bank // 4) % 4, bank // 16
    z, core = z_hi * 4 + lane // 2, lane % 2
    xy = y * 4 + x

    def z_peer(step):
        there = (z + step) % 8
        return there, ((there // 4) * 16 + xy, (there % 4) * 2 + core)

    def xy_peer(step):
        there = ((y + step[1]) % 4) * 4 + (x + step[0]) % 4
        return there, (z_hi * 16 + there, lane)

    partner = (bank, (lane // 2) * 2 + 1 - core)
    z_peers = [z_peer(step) for step in Z_STEPS]
    xy_peers = [xy_peer(step) for step in XY_STEPS]

    barrier = pltpu.get_barrier_semaphore()
    for _, device in xy_peers[:5] + z_peers + xy_peers[5:]:
        pl.semaphore_signal(barrier, inc=1, device_id=device, device_id_type=MESH)
    pl.semaphore_signal(barrier, inc=1, device_id=partner, device_id_type=MESH)
    loads = [
        pltpu.make_async_copy(src, dst, in_sem.at[k])
        for k, (src, dst) in enumerate(
            ((energies_in, energies), (mixes_in, mixes), (phases_in, phases), (amps_in, amps))
        )
    ]
    for load in loads:
        load.start()

    sent = []

    def remote(src, dst, stage, device):
        return pltpu.make_async_remote_copy(
            src_ref=src, dst_ref=dst, send_sem=send_sem.at[stage], recv_sem=recv_sem.at[stage],
            device_id=device, device_id_type=MESH,
        )

    def all_of(ref, sem):
        return pltpu.make_async_copy(ref, ref, sem)

    def arrived(ref, stage):
        with jax.named_scope(f"w{stage}"):
            all_of(ref, recv_sem.at[stage]).wait()

    def send_z(src, dst, stage):
        for there, device in z_peers:
            remote(src.at[there], dst.at[z], stage, device).start()
        dst[z] = src[z]
        sent.append((src.at[pl.ds(0, 7)], stage))

    def send_xy(src, dst, stage, unit):
        own = pl.ds(xy * unit, unit)
        for there, device in xy_peers:
            remote(src.at[:, pl.ds(there * unit, unit), :], dst.at[:, own, :], stage, device).start()
        dst[:, own, :] = src[:, own, :]
        sent.append((src.at[:, pl.ds(0, 15 * unit), :], stage))

    def level_z(src, dst, q, stage):
        pair = pl.ds(q, 2)
        for there, device in z_peers:
            remote(src.at[pair, there], dst.at[pair, z], stage, device).start()
        dst[pair, z] = src[pair, z]
        sent.append((src.at[pair, pl.ds(0, 7)], stage))

    def level_xy(src, dst, q, stage):
        pair, own = pl.ds(q, 2), pl.ds(xy, 1)
        for there, device in xy_peers:
            remote(src.at[pair, :, pl.ds(there, 1), :], dst.at[pair, :, own, :], stage, device).start()
        dst[pair, :, own, :] = src[pair, :, own, :]
        sent.append((src.at[pair, :, pl.ds(0, 15), :], stage))

    def swap(src, dst, stage):
        remote(src, dst, stage, partner).start()
        sent.append((src, stage))

    def came_z(buf, stage):
        arrived(buf.at[pl.ds(0, 7)], stage)

    def came_xy(buf, stage, unit):
        arrived(buf.at[:, pl.ds(0, 15 * unit), :], stage)

    E1, E2, S1, S2, D1, D2, T1, T2, P1, P2 = 0, 4, 8, 12, 16, 20, 24, 28, 32, 34

    loads[0].wait()
    for q in range(4):
        for sz in range(8):
            e_send[q, sz] = energies[sz // 2, pl.ds((sz % 2) * 64 + q, 16, stride=4), :]
    loads[1].wait()
    mix_sin, mix_cos = sine_cosine(mixes[...])

    def cs(layer, group, shape):
        at = (slice(layer, layer + 1), slice(group, group + 1))
        return jnp.broadcast_to(mix_cos[at], shape), jnp.broadcast_to(mix_sin[at], shape)

    row = lax.broadcasted_iota(jnp.int32, (128, 128), 0)
    column = lax.broadcasted_iota(jnp.int32, (128, 128), 1)
    apart = row ^ column

    def build(slot, layer, groups, on_left):
        size, count = None, None
        for k, group in enumerate(groups):
            c, s = cs(layer, group, (128, 128))
            bit = (apart >> k) & 1
            factor = jnp.where(bit == 1, s, c)
            size = factor if size is None else size * factor
            count = bit if count is None else count + bit
        odd = (count & 1) == 1
        sign = 1.0 - (count & 2).astype(F32)
        re = jnp.where(odd, 0.0, size * sign)
        im = jnp.where(odd, -size * sign, 0.0)
        for half, (real, imag) in enumerate(zip(split(re), split(im))):
            tables[slot, half, 0:128, 0:128] = real
            tables[slot, half, 128:256, 128:256] = real
            tables[slot, half, 0:128, 128:256] = -imag if on_left else imag
            tables[slot, half, 128:256, 0:128] = imag if on_left else -imag

    def table(slot):
        return tables[slot, 0], tables[slot, 1]

    lanes = (0,) * 7
    rows = (1,) * 5 + (2, 2)
    chips = (2,) * 4 + (3, 3) + (2,)
    build(0, 0, lanes, False)
    build(1, 0, rows, True)

    with jax.named_scope("barrier"):
        pl.semaphore_wait(barrier, 23)
    level_z(e_send, e_mid, 0, E1)
    level_xy(e_send, e_mid, 2, E1 + 2)

    for load in loads[2:]:
        load.wait()

    def turned(re, im, levels, layer):
        angle = jnp.broadcast_to(phases[layer:layer + 1, :], levels.shape) * levels
        s, c = sine_cosine(angle)
        return re * c + im * s, im * c - re * s

    def mixed(u, v, c, s):
        (ur, ui), (vr, vi) = u, v
        return (c * ur + s * vi, c * ui - s * vr), (c * vr + s * ui, c * vi - s * ur)

    c1, s1 = cs(0, 1, (32, 128))
    for t in range(4):
        parts = {}
        for q in range(4):
            at = pl.ds(q, 32, stride=4)
            parts[q] = turned(amps[0, t, at, :], amps[1, t, at, :], energies[t, at, :], 0)
        for low, high in ((0, 1), (2, 3), (0, 2), (1, 3)):
            parts[low], parts[high] = mixed(parts[low], parts[high], c1, s1)
        for q in range(4):
            for part in range(2):
                canon[q, t * 32:t * 32 + 32, part * 128:part * 128 + 128] = parts[q][part]
    for q in ORDER:
        done = times(split(canon[q]), table(0))
        moved[q, 0:128, :] = done[:, 0:128]
        moved[q, 128:256, :] = done[:, 128:256]
        swap(moved.at[q], other.at[q], D1 + q)

    def core_mixed(near, far, q, layer):
        c, s = cs(layer, 3, (128, 128))
        re = c * near[q, 0:128, :] + s * far[q, 128:256, :]
        im = c * near[q, 128:256, :] - s * far[q, 0:128, :]
        return jnp.concatenate([re, im], axis=0)

    def spread(buf, q, value):
        for sz in range(8):
            for part in range(2):
                at = part * 128 + sz * 16
                buf[q, sz, pl.ds(part, 16, stride=2), :] = value[at:at + 16, :]

    def gathered(buf, q):
        return jnp.concatenate(
            [buf[q, sz, pl.ds(part, 16, stride=2), :] for part in range(2) for sz in range(8)], axis=0
        )

    for q in ORDER:
        arrived(other.at[q], D1 + q)
        spread(s_buf, q, times(table(1), split(core_mixed(moved, other, q, 0))))
        if q in Z_FIRST:
            send_z(s_buf.at[q], s_mid.at[q], S1 + q)
        else:
            send_xy(s_buf.at[q], s_mid.at[q], S1 + q, 2)
    build(2, 0, chips, True)

    arrived(e_mid.at[pl.ds(2, 2), :, pl.ds(0, 15), :], E1 + 2)
    level_z(e_mid, e_got, 2, E2 + 2)
    arrived(e_mid.at[pl.ds(0, 2), pl.ds(0, 7)], E1)
    level_xy(e_mid, e_got, 0, E2)
    build(3, 1, chips, True)
    build(4, 1, lanes, False)
    build(5, 1, rows, True)

    def forward(q):
        if q in Z_FIRST:
            came_z(s_mid.at[q], S1 + q)
            send_xy(s_mid.at[q], s_got.at[q], S2 + q, 2)
        else:
            came_xy(s_mid.at[q], S1 + q, 2)
            send_z(s_mid.at[q], s_got.at[q], S2 + q)

    def middle(q):
        if q in Z_FIRST:
            if q == 0:
                arrived(e_got.at[pl.ds(0, 2), :, pl.ds(0, 15), :], E2)
            came_xy(s_got.at[q], S2 + q, 2)
        else:
            if q == 2:
                arrived(e_got.at[pl.ds(2, 2), pl.ds(0, 7)], E2 + 2)
            came_z(s_got.at[q], S2 + q)
        value = times(table(2), split(gathered(s_got, q)))
        levels = jnp.concatenate([e_got[q, sz] for sz in range(8)], axis=0)
        value = jnp.concatenate(turned(value[0:128, :], value[128:256, :], levels, 1), axis=1)
        value = times(split(value), table(4))
        value = jnp.concatenate([value[:, 0:128], value[:, 128:256]], axis=0)
        held[q] = times(table(3), split(value))
        swap(held.at[q], held_far.at[q], D2 + q)

    def back(q):
        arrived(held_far.at[q], D2 + q)
        spread(t_buf, q, core_mixed(held, held_far, q, 1))
        if q in Z_FIRST:
            send_z(t_buf.at[q], t_mid.at[q], T1 + q)
        else:
            send_xy(t_buf.at[q], t_mid.at[q], T1 + q, 2)

    def home(q):
        if q in Z_FIRST:
            came_z(t_mid.at[q], T1 + q)
            send_xy(t_mid.at[q], t_got.at[q], T2 + q, 2)
        else:
            came_xy(t_mid.at[q], T1 + q, 2)
            send_z(t_mid.at[q], t_got.at[q], T2 + q)

    def final(q):
        if q in Z_FIRST:
            came_xy(t_got.at[q], T2 + q, 2)
        else:
            came_z(t_got.at[q], T2 + q)
        last[q] = times(table(5), split(gathered(t_got, q)))

    cr, sr = cs(1, 1, (128, 128))

    def pair(low, high):
        first, second = mixed(
            (last[low, 0:128, :], last[low, 128:256, :]), (last[high, 0:128, :], last[high, 128:256, :]), cr, sr
        )
        for q, value in ((low, first), (high, second)):
            last[q, 0:128, :], last[q, 128:256, :] = value

    forward(0)
    forward(2)
    forward(3)
    forward(1)
    middle(0)
    back(0)
    middle(1)
    middle(2)
    back(1)
    back(2)
    middle(3)
    back(3)
    home(0)
    home(2)
    home(1)
    home(3)
    final(0)
    final(2)
    pair(0, 2)
    final(1)
    final(3)
    pair(1, 3)
    pair(0, 1)
    pair(2, 3)

    for q in range(4):
        chance = last[q, 0:128, :] * last[q, 0:128, :] + last[q, 128:256, :] * last[q, 128:256, :]
        for t in range(4):
            for r6 in range(2):
                at = t * 32 + r6 * 16
                p_send[r6, pl.ds(t * 4 + q, 16, stride=16), :] = chance[at:at + 16, :]
    for half, stage in ((1 - z_hi, P1), (z_hi, P1 + 1)):
        for there, device in xy_peers:
            remote(
                p_send.at[half, pl.ds(pl.multiple_of(there * 16, 16), 16), :], p_got.at[stage - P1, xy], stage, device
            ).start()
        p_got[stage - P1, xy] = p_send[half, pl.ds(pl.multiple_of(xy * 16, 16), 16), :]
        sent.append((p_got.at[stage - P1, pl.ds(0, 15)], stage))
    for q in range(4):
        for part in range(2):
            for t in range(4):
                at = part * 128 + t * 32
                out[part, t, pl.ds(q, 32, stride=4), :] = last[q, at:at + 32, :]

    def summed(half):
        arrived(p_got.at[half, pl.ds(0, 15)], P1 + half)
        parts = [p_got[half, k] for k in range(16)]
        while len(parts) > 1:
            parts = [parts[k] + parts[k + 1] for k in range(0, len(parts), 2)]
        return parts[0]

    p_sum[...] = summed(0)
    remote(p_sum, p_far, P2, ((1 - z_hi) * 16 + xy, lane)).start()
    near = summed(1)
    for buf, stage in sent:
        all_of(buf, send_sem.at[stage]).wait()
    arrived(p_far, P2)
    marg[...] = (near + p_far[...]) * (1.0 / 32.0)
    all_of(p_far, send_sem.at[P2]).wait()


def writer(parts, chance, parts_out, chance_out, staged, sem):
    copies = [pltpu.make_async_copy(parts, parts_out, sem.at[0]), pltpu.make_async_copy(staged, chance_out, sem.at[1])]
    copies[0].start()
    for t in range(4):
        staged[t] = chance[t * 4:t * 4 + 4, :]
    copies[1].start()
    for copy in copies:
        copy.wait()


def on_device(amplitudes, energies, phase_angles, mix_angles):
    vmem = pl.BlockSpec(memory_space=pltpu.VMEM)
    state = pltpu.VMEM((4, 8, 32, 128), F32)
    levels = pltpu.VMEM((4, 8, 16, 128), F32)
    tall = pltpu.VMEM((4, 256, 128), F32)
    parts, chance = pl.pallas_call(
        kernel,
        out_shape=(
            jax.ShapeDtypeStruct((2, 4, 128, 128), F32),
            jax.ShapeDtypeStruct((16, 128), F32),
        ),
        in_specs=[pl.BlockSpec(memory_space=pltpu.HBM)] * 4,
        out_specs=(vmem, vmem),
        scratch_shapes=[
            pltpu.VMEM((2, 4, 128, 128), F32),
            pltpu.VMEM((4, 128, 128), F32),
            pltpu.VMEM((2, 128), F32),
            pltpu.VMEM((2, 4), F32),
            pltpu.SemaphoreType.DMA((4,)),
            pltpu.VMEM((6, 2, 256, 256), BF16),
            pltpu.VMEM((4, 128, 256), F32),
            tall, tall,
            levels, levels, levels,
            state, state, state,
            tall, tall,
            state, state, state,
            tall,
            pltpu.VMEM((2, 256, 128), F32),
            pltpu.VMEM((2, 16, 16, 128), F32),
            pltpu.VMEM((16, 128), F32),
            pltpu.VMEM((16, 128), F32),
            pltpu.SemaphoreType.DMA((STAGES,)),
            pltpu.SemaphoreType.DMA((STAGES,)),
        ],
        compiler_params=pltpu.CompilerParams(
            collective_id=0, has_side_effects=True, vmem_limit_bytes=48 * 1024 * 1024
        ),
    )(*[pltpu.with_memory_space_constraint(a, pltpu.HBM) for a in (amplitudes, energies, phase_angles, mix_angles)])
    hbm = pl.BlockSpec(memory_space=pltpu.HBM)
    return pl.pallas_call(
        writer,
        out_shape=(
            jax.ShapeDtypeStruct((2, 4, 128, 128), F32),
            jax.ShapeDtypeStruct((4, 4, 128), F32),
        ),
        in_specs=[vmem] * 2,
        out_specs=(hbm, hbm),
        scratch_shapes=[pltpu.VMEM((4, 4, 128), F32), pltpu.SemaphoreType.DMA((2,))],
        compiler_params=pltpu.CompilerParams(vmem_limit_bytes=1024 * 1024),
    )(parts, chance)


def solution(mesh):
    placed = (P(None, ("bank", "lane"), None, None), P(("bank", "lane"), None, None), P(), P())
    return jax.shard_map(
        on_device,
        mesh=mesh,
        in_specs=placed,
        out_specs=(P(None, ("bank", "lane"), None, None), P("lane", "bank", None)),
        check_vma=False,
    )
```
